32 devices in a mesh: member: 2 (over x), fsdp: 16 (over z, y, core).
Axes of the slice: x: 2, y: 2, z: 4, core: 2. Of those that a mesh axis runs over, the one named last changes fastest.
Arguments:
- latents: bfloat16 [2, 32768, 512], P('member', 'fsdp'), may hold values from -6 to 6
- noise: float32 [2, 32], P('member'), may hold values from -4 to 4
- cond_gain: float32 [32, 512], replicated, may hold values from -0.5 to 0.5
- cond_shift: float32 [32, 512], replicated, may hold values from -0.5 to 0.5
- w_in: bfloat16 [512, 2048], P('fsdp'), may hold values from -0.25 to 0.25
- b_in: float32 [2048], replicated, may hold values from -3 to 3
- w_out: bfloat16 [2048, 512], P('fsdp'), may hold values from -0.125 to 0.125
- target: bfloat16 [32768, 512], P('fsdp'), may hold values from -6 to 6
Outputs:
- prediction: bfloat16 [2, 32768, 512], P('member', 'fsdp')
- grad_in: float32 [512, 2048], P('fsdp')
- grad_out: float32 [2048, 512], P('fsdp')
- crps_mean: float32 [], replicated
The draws below stay inside these ranges and needn't reach their ends.
All inputs are finite; a program needn't handle non-finite values.
Results may differ from the reference program's by a relative error of at most 0.0043.
Values may be sent and summed in bfloat16 or wider, within the bound.
A program may use at most 128 MiB of HBM per device.

```python
import jax
import jax.numpy as jnp
from jax import lax

D = 512
H = 2048
ZN = 32
ROWS = 2048
NODES = 32768


def with_spikes(entries, stream_key, source, target, shards_of, factor):
    owner, partner = [(jnp.arange(entries.shape[axis_at]) // (entries.shape[axis_at] // shards_of)).reshape([-1 if axis == axis_at else 1 for axis in range(entries.ndim)]) for axis_at in (source, target)]
    chosen = jax.random.permutation(stream_key, shards_of)[partner]
    strong = (owner == chosen) | (owner == (partner + shards_of // 2) % shards_of)
    return jnp.where(strong, factor * entries, entries)


def levels(key, extent, shards, smallest, top_value):
    def one(position, blocks):
        heights = jax.random.uniform(jax.random.fold_in(jax.random.fold_in(key, 6), position), (blocks,), jnp.float32, smallest / len(shards), top_value / len(shards))
        return jnp.repeat(jnp.exp(heights), extent[position] // blocks).reshape((-1,) + (1,) * (len(extent) - position - 1))

    factor_of = one(*shards[0])
    for cut in shards[1:]:
        factor_of = factor_of * one(*cut)
    return factor_of


def centred(stream_key, dims, scale, bound, pieces=(), kind=jnp.bfloat16):
    result = scale * jax.random.normal(stream_key, dims, jnp.float32)
    if pieces:
        result = result * levels(stream_key, dims, pieces, -0.22, 0.18)
    return jnp.clip(result, -bound, bound).astype(kind)


def heavy_noise(stream_key, extent, width, most, split, heavy, kind=jnp.bfloat16):
    array = width * jax.random.normal(stream_key, extent, jnp.float32)
    if split:
        array = array * levels(stream_key, extent, split, -0.22, 0.18)
    return jnp.clip(with_spikes(array, jax.random.fold_in(stream_key, 3), *heavy), -most, most).astype(kind)


def setup_inputs(seed: int = 0) -> dict:
    key_list = jax.random.split(jax.random.key(seed), 9)
    return {
        "latents": heavy_noise(key_list[0], (2, NODES, D), 1.0, 6.0, ((0, 2), (1, 16)), (1, 2, 16, 2.0)),
        "noise": centred(key_list[1], (2, ZN), 1.0, 4.0, ((0, 2),), jnp.float32),
        "cond_gain": centred(key_list[2], (ZN, D), (4 * ZN) ** -0.5, 0.5, (), jnp.float32),
        "cond_shift": centred(key_list[3], (ZN, D), (4 * ZN) ** -0.5, 0.5, (), jnp.float32),
        "w_in": centred(key_list[4], (D, H), D ** -0.5, 0.25, ((0, 16),)),
        "b_in": centred(key_list[5], (H,), 0.5, 3.0, (), jnp.float32),
        "w_out": centred(key_list[6], (H, D), H ** -0.5, 0.125, ((0, 16),)),
        "target": centred(key_list[7], (NODES, D), 1.0, 6.0, ((0, 16),)),
    }


COEF = 0.7978845608
CUBIC = 0.044715

def gelu_value(v):
    return 0.5 * v * (1.0 + jnp.tanh(COEF * (v + CUBIC * v * v * v)))

def gelu_slope(v):
    u = jnp.tanh(COEF * (v + CUBIC * v * v * v))
    return 0.5 * (1.0 + u) + 0.5 * v * (1.0 - u * u) * COEF * (1.0 + 3.0 * CUBIC * v * v)

def smooth(d):
    return jnp.sqrt(d * d + 0.0625)

def forward(block, noise_row, cond_gain, cond_shift, w_in, b_in):
    gain = 1.0 + jnp.dot(noise_row[None, :], cond_gain, precision=lax.Precision.HIGHEST, preferred_element_type=jnp.float32)[0]
    shift = jnp.dot(noise_row[None, :], cond_shift, precision=lax.Precision.HIGHEST, preferred_element_type=jnp.float32)[0]
    values = block.astype(jnp.float32)
    center = lax.optimization_barrier(jnp.mean(values, axis=1, keepdims=True))
    spread = lax.optimization_barrier(jnp.mean((values - center) ** 2, axis=1, keepdims=True))
    normed = ((values - center) / jnp.sqrt(spread + 0.25) * gain + shift).astype(jnp.bfloat16)
    pre = jnp.dot(normed, w_in, preferred_element_type=jnp.float32) + b_in
    act = gelu_value(pre).astype(jnp.bfloat16)
    return (normed, pre, act, values)

def reference(latents, noise, cond_gain, cond_shift, w_in, b_in, w_out, target):
    count = NODES // ROWS
    blocks = latents.reshape(2, count, ROWS, D)
    targets = target.reshape(count, ROWS, D)
    scale = 1.0 / jnp.sqrt(jnp.float32(2 * NODES))

    def predict(member):

        def one(block):
            normed, pre, act, values = forward(block, noise[member], cond_gain, cond_shift, w_in, b_in)
            return (values + jnp.dot(act, w_out, preferred_element_type=jnp.float32)).astype(jnp.bfloat16)
        return lax.map(one, blocks[member])
    preds = jnp.stack([predict(0), predict(1)])

    def accumulate(carry, items):
        grad_a, grad_b, total = carry
        first, second, tgt, pred_a, pred_b = items
        owns = [pred_a.astype(jnp.float32), pred_b.astype(jnp.float32)]
        tval = tgt.astype(jnp.float32)
        for member, block in ((0, first), (1, second)):
            normed, pre, act, values = forward(block, noise[member], cond_gain, cond_shift, w_in, b_in)
            mine = owns[member]
            other = owns[1 - member]
            near = mine - tval
            apart = mine - other
            total = total + jnp.sum(0.5 * smooth(near) - 0.25 * smooth(apart))
            dpred = ((0.5 * near / smooth(near) - 0.5 * apart / smooth(apart)) * scale).astype(jnp.bfloat16)
            dact = jnp.dot(dpred, w_out.T, preferred_element_type=jnp.float32)
            dpre = (dact * gelu_slope(pre)).astype(jnp.bfloat16)
            grad_a = grad_a + jnp.dot(normed.T, dpre, preferred_element_type=jnp.float32)
            grad_b = grad_b + jnp.dot(act.T, dpred, preferred_element_type=jnp.float32)
        return ((grad_a, grad_b, total), None)
    start = (jnp.zeros((D, H), jnp.float32), jnp.zeros((H, D), jnp.float32), jnp.zeros((), jnp.float32))
    (grad_in, grad_out, total), unused = lax.scan(accumulate, start, (blocks[0], blocks[1], targets, preds[0], preds[1]))
    crps_mean = total / jnp.float32(2 * NODES * D)
    return (preds.reshape(2, NODES, D), grad_in, grad_out, crps_mean)
```

```python
import functools

import jax
import jax.numpy as jnp
from jax import lax
from jax.experimental import pallas as pl
from jax.experimental.pallas import tpu as pltpu
from jax.sharding import PartitionSpec as P

COEF = 0.7978845608
CUBIC = 0.044715


def swapped(block, axis, apart):
    count = lax.axis_size(axis)
    route = []
    for low in range(count):
        high = low | 1 << apart
        if high != low and high < count:
            route += [(low, high), (high, low)]
    return lax.ppermute(block, axis, route)


def gelu_value(v):
    return 0.5 * v * (1.0 + jnp.tanh(COEF * (v + CUBIC * v * v * v)))


def gelu_slope(v):
    u = jnp.tanh(COEF * (v + CUBIC * v * v * v))
    return 0.5 * (1.0 + u) + 0.5 * v * (1.0 - u * u) * COEF * (1.0 + 3.0 * CUBIC * v * v)


def smooth(d):
    return jnp.sqrt(d * d + 0.0625)


def general(latents, noise, cond_gain, cond_shift, w_in, b_in, w_out, target):
    block = latents[0]
    noise_row = noise[0]
    rows = block.shape[0]
    width = block.shape[1]
    groups = lax.axis_size("fsdp")
    nodes = rows * groups
    gain = (
        1.0
        + jnp.dot(
            noise_row[None, :],
            cond_gain,
            precision=lax.Precision.HIGHEST,
            preferred_element_type=jnp.float32,
        )[0]
    )
    shift = jnp.dot(
        noise_row[None, :],
        cond_shift,
        precision=lax.Precision.HIGHEST,
        preferred_element_type=jnp.float32,
    )[0]
    values = block.astype(jnp.float32)
    center = jnp.mean(values, axis=1, keepdims=True)
    spread = jnp.mean((values - center) ** 2, axis=1, keepdims=True)
    normed = ((values - center) / jnp.sqrt(spread + 0.25) * gain + shift).astype(jnp.bfloat16)
    columns = normed
    pre = (
        jnp.dot(
            columns,
            lax.all_gather(w_in, "fsdp", axis=0, tiled=True),
            preferred_element_type=jnp.float32,
        )
        + b_in
    )
    act = gelu_value(pre).astype(jnp.bfloat16)
    columns = act
    output = values + jnp.dot(
        columns,
        lax.all_gather(w_out, "fsdp", axis=0, tiled=True),
        preferred_element_type=jnp.float32,
    )
    prediction = output.astype(jnp.bfloat16)
    partner = swapped(prediction, "member", 0)
    mine = prediction.astype(jnp.float32)
    near = mine - target.astype(jnp.float32)
    apart = mine - partner.astype(jnp.float32)
    local_sum = jnp.sum(0.5 * smooth(near) - 0.25 * smooth(apart))
    crps_mean = lax.psum(local_sum, ("member", "fsdp")) / jnp.float32(2 * nodes * width)
    scale = 1.0 / jnp.sqrt(jnp.float32(2 * nodes))
    dpred = ((0.5 * near / smooth(near) - 0.5 * apart / smooth(apart)) * scale).astype(jnp.bfloat16)
    across = (((1,), (1,)), ((), ()))
    dact = lax.dot_general(
        dpred,
        lax.all_gather(w_out, "fsdp", axis=0, tiled=True),
        across,
        preferred_element_type=jnp.float32,
    )
    dpre = (dact * gelu_slope(pre)).astype(jnp.bfloat16)
    contract = (((0,), (0,)), ((), ()))
    columns = normed
    shard_in = lax.psum_scatter(
        lax.dot_general(columns, dpre, contract, preferred_element_type=jnp.float32),
        "fsdp",
        scatter_dimension=0,
        tiled=True,
    )
    columns = act
    shard_out = lax.psum_scatter(
        lax.dot_general(columns, dpred, contract, preferred_element_type=jnp.float32),
        "fsdp",
        scatter_dimension=0,
        tiled=True,
    )
    grad_in, grad_out = lax.psum((shard_in, shard_out), "member")
    return (prediction[None], grad_in, grad_out, crps_mean)


TILE = 256
WIDE = 512
MESH = pl.DeviceIdType.MESH


def fused_kernel(
    n, gs_in, lat, b_in, w_in, w_out, target,
    pred, gin, gout, crps,
    win_s, wout_s, x_s, t_s, gs_s, p_s, norm_t, norm_s, act_s, slope_s, dp_s, dp_t, dpre_s, cr_s,
    pair_tx, pair_rx, ring_tx, ring_rx, mine_s, gin_tx, gout_tx, gin_rx, gout_rx, cr_tx, cr_rx,
    g_send, g_recv, q_send, q_recv, l_send, l_recv, local_sem, p_send, p_recv, o_sem,
    pair_ss, pair_rs, ring_ss, ring_rs, fin_ss, fin_rs, out_ss, out_rs, cr_ss, cr_rs,
):
    m = lax.axis_index("member")
    f = lax.axis_index("fsdp")
    chips = n // 2
    core = f % 2
    chip = f // 2
    turn = 1 - 2 * core

    def chip_at(place):
        low = place < chips // 2
        return jnp.where(low, 2 * place, 2 * (chips - 1 - place) + 1)

    position = jnp.where(chip % 2 == 0, chip // 2, chips - 1 - chip // 2)

    def place(offset):
        return (position + turn * offset + 2 * chips) % chips

    following = (m, 2 * chip_at(place(1)) + core)
    twin = (m, 2 * chip + 1 - core)
    partner = (1 - m, f)
    flat = m * n + f
    total = 2 * n

    def device(index):
        return (index // n, index % n)

    barrier = pltpu.get_barrier_semaphore()

    @pl.loop(1, total)
    def greet(k):
        pl.semaphore_signal(barrier, inc=1, device_id=device((flat + k) % total), device_id_type=MESH)

    pl.semaphore_wait(barrier, total - 1)

    def remote(src, dst, send, recv, to):
        return pltpu.make_async_remote_copy(
            src_ref=src, dst_ref=dst, send_sem=send, recv_sem=recv, device_id=to, device_id_type=MESH
        )

    half = x_s.shape[1]
    width = x_s.shape[2]
    hidden = win_s.shape[1]
    rin = w_in.shape[0]
    rout = w_out.shape[0]
    mine_from = pl.multiple_of(m * half, half)
    other_from = pl.multiple_of((1 - m) * half, half)

    def slot(which, owner):
        if which == 0:
            return win_s.at[pl.ds(pl.multiple_of(owner * rin, rin), rin)]
        return wout_s.at[pl.ds(pl.multiple_of(owner * rout, rout), rout)]

    def ring_copy(which, step, src, owner):
        return remote(src, slot(which, owner), g_send.at[which, step], g_recv.at[which, step], following)

    def pair_copy(which, step, src, owner):
        return remote(src, slot(which, owner), q_send.at[which, step], q_recv.at[which, step], twin)

    shards = (w_in, w_out)
    for which in range(2):
        ring_copy(which, 0, shards[which], f).start()
    swap = remote(lat.at[pl.ds(other_from, half)], x_s.at[0], l_send.at[0], l_recv.at[0], partner)
    swap.start()
    gs_swap = remote(gs_in, gs_s.at[0], l_send.at[1], l_recv.at[1], partner)
    gs_swap.start()
    for which in range(2):
        pair_copy(which, 0, shards[which], f).start()
    keep = pltpu.make_async_copy(lat.at[pl.ds(mine_from, half)], x_s.at[1], local_sem.at[0])
    keep.start()
    goal = pltpu.make_async_copy(target.at[pl.ds(mine_from, half)], t_s, local_sem.at[1])
    goal.start()
    gs_s[1] = gs_in[...]
    cr_s[...] = jnp.zeros_like(cr_s)
    win_s[pl.ds(pl.multiple_of(f * rin, rin), rin), :] = w_in[...]
    wout_s[pl.ds(pl.multiple_of(f * rout, rout), rout), :] = w_out[...]

    for step in range(1, chips):
        owner = 2 * chip_at(place(-step)) + core
        for which in range(2):
            ring_copy(which, step - 1, slot(which, owner), owner).wait_recv()
            if step < chips - 1:
                ring_copy(which, step, slot(which, owner), owner).start()
            pair_copy(which, step, slot(which, owner), owner).start()
    for step in range(chips):
        owner = 2 * chip_at(place(step)) + 1 - core
        for which in range(2):
            pair_copy(which, step, slot(which, owner), owner).wait_recv()
    for step in range(chips):
        owner = 2 * chip_at(place(-step)) + core
        for which in range(2):
            src = shards[which] if step == 0 else slot(which, owner)
            if step < chips - 1:
                ring_copy(which, step, src, owner).wait_send()
            pair_copy(which, step, src, owner).wait_send()
    keep.wait()
    goal.wait()
    gs_swap.wait()
    swap.wait()

    tiles = half // TILE
    scale = (1.0 / (2.0 * n * 2 * half) ** 0.5)

    def home(tile):
        start = pl.multiple_of(tile * TILE, TILE)
        there = pl.multiple_of(m * half + tile * TILE, TILE)
        back = remote(p_s.at[0, pl.ds(start, TILE)], pred.at[pl.ds(there, TILE)], p_send.at[tile], p_recv.at[tile], partner)
        here = pltpu.make_async_copy(p_s.at[1, pl.ds(start, TILE)], pred.at[pl.ds(there, TILE)], o_sem.at[tile])
        return back, here

    def arrival(tile):
        start = pl.multiple_of(tile * TILE, TILE)
        there = pl.multiple_of((1 - m) * half + tile * TILE, TILE)
        return remote(p_s.at[0, pl.ds(start, TILE)], pred.at[pl.ds(there, TILE)], p_send.at[tile], p_recv.at[tile], partner)

    @pl.loop(0, tiles)
    def nodes(tile):
        start = pl.multiple_of(tile * TILE, TILE)
        base = pl.multiple_of(tile * 2 * TILE, 2 * TILE)
        rows = pl.ds(base, 2 * TILE)
        for side in range(2):
            values = x_s[side, pl.ds(start, TILE), :].astype(jnp.float32)
            center = jnp.mean(values, axis=1, keepdims=True)
            moved = values - center
            spread = jnp.mean(moved * moved, axis=1, keepdims=True)
            normed = moved * lax.rsqrt(spread + 0.25) * gs_s[side, 0:1, :] + gs_s[side, 1:2, :]
            normed = normed.astype(jnp.bfloat16)
            norm_s[side * TILE : (side + 1) * TILE, :] = normed
        norm_t[:, rows] = norm_s[...].T
        for j in range(hidden // WIDE):
            cols = slice(j * WIDE, (j + 1) * WIDE)
            v = jnp.dot(norm_s[...], win_s[:, cols], preferred_element_type=jnp.float32) + b_in[:, cols]
            square = v * v
            u = jnp.tanh(COEF * (v + CUBIC * square * v))
            gate = 0.5 * (1.0 + u)
            act_s[rows, cols] = (v * gate).astype(jnp.bfloat16)
            slope_s[:, cols] = gate + (0.5 * COEF) * v * (1.0 - u * u) * (1.0 + 3.0 * CUBIC * square)
        out = jnp.dot(act_s[rows, :], wout_s[...], preferred_element_type=jnp.float32)
        guess = []
        for side in range(2):
            value = x_s[side, pl.ds(start, TILE), :].astype(jnp.float32) + out[side * TILE : (side + 1) * TILE]
            value = value.astype(jnp.bfloat16)
            p_s[side, pl.ds(start, TILE), :] = value
            guess.append(value.astype(jnp.float32))
        goal_tile = t_s[pl.ds(start, TILE), :].astype(jnp.float32)
        slopes = []
        value_sum = None
        for d, weight in ((guess[0] - goal_tile, 0.5), (guess[1] - goal_tile, 0.5), (guess[0] - guess[1], -0.5)):
            q = d * d + 0.0625
            r = lax.rsqrt(q)
            slopes.append(0.5 * d * r)
            term = weight * (q * r)
            value_sum = term if value_sum is None else value_sum + term
        cr_s[...] += jnp.sum(value_sum.reshape(TILE // 8, 8, width), axis=0)
        dp_s[:TILE, :] = ((slopes[0] - slopes[2]) * scale).astype(jnp.bfloat16)
        dp_s[TILE:, :] = ((slopes[1] + slopes[2]) * scale).astype(jnp.bfloat16)
        dp_t[:, rows] = dp_s[...].T
        for j in range(hidden // WIDE):
            cols = slice(j * WIDE, (j + 1) * WIDE)
            dact = lax.dot_general(
                dp_s[...], wout_s[cols, :], (((1,), (1,)), ((), ())), preferred_element_type=jnp.float32
            )
            dpre_s[rows, cols] = (dact * slope_s[:, cols]).astype(jnp.bfloat16)
        back, here = home(tile)
        back.start()
        here.start()

    part = cr_s[:, 0:128]
    for j in range(1, width // 128):
        part = part + cr_s[:, j * 128 : (j + 1) * 128]
    cr_tx[...] = part
    cr_rx[flat] = part

    def cr_copy(to, source):
        return remote(cr_tx, cr_rx.at[source], cr_ss.at[to], cr_rs.at[source], device(to))

    cw = hidden // n

    def columns(owner):
        return pl.ds(pl.multiple_of(owner * cw, cw), cw)

    def pair_sum(which, step):
        return remote(
            pair_tx.at[step, which], pair_rx.at[step, which], pair_ss.at[step, which], pair_rs.at[step, which], twin
        )

    def ring_sum(which, step):
        return remote(
            ring_tx.at[step, which], ring_rx.at[step, which], ring_ss.at[step, which], ring_rs.at[step, which], following
        )

    def compute(step):
        own = columns(2 * chip_at(place(-step - 1)) + core)
        twins = columns(2 * chip_at(place(step + 1)) + 1 - core)
        for which, (left, right) in enumerate(((norm_t, dpre_s), (dp_t, act_s))):
            both = jnp.concatenate([right[:, own], right[:, twins]], axis=1)
            product = jnp.dot(left[...], both, preferred_element_type=jnp.float32)
            mine_s[step, which] = product[:, :cw]
            pair_tx[step, which] = product[:, cw:].astype(jnp.bfloat16)
        for which in range(2):
            pair_sum(which, step).start()

    def finish(step, first=False, last=False):
        for which in range(2):
            pair_sum(which, step).wait_recv()
            value = mine_s[step, which] + pair_rx[step, which].astype(jnp.float32)
            if not first:
                ring_sum(which, step - 1).wait_recv()
                value = value + ring_rx[step - 1, which].astype(jnp.float32)
            value = value.astype(jnp.bfloat16)
            if not last:
                ring_tx[step, which] = value
                ring_sum(which, step).start()
            elif which == 0:
                gin_tx[...] = value
            else:
                gout_tx[...] = value

    compute(0)
    compute(1)
    finish(0, first=True)

    @pl.loop(1, chips - 1)
    def steps(step):
        compute(step + 1)
        finish(step)

    @pl.loop(1, total)
    def tell(k):
        cr_copy((flat + k) % total, flat).start()

    finish(chips - 1, last=True)

    def fin_copy(to, source):
        target_rows = pl.ds(pl.multiple_of((to % n) * rin, rin), rin)
        return remote(gin_tx.at[target_rows], gin_rx.at[source], fin_ss.at[to], fin_rs.at[source], device(to))

    out_copy = remote(gout_tx, gout_rx, out_ss, out_rs, partner)
    out_copy.start()

    @pl.loop(1, total)
    def scatter(k):
        fin_copy((flat + k) % total, flat).start()

    gin_rx[flat] = gin_tx[pl.ds(pl.multiple_of(f * rin, rin), rin), :]

    @pl.loop(1, total)
    def heard(k):
        cr_copy(flat, (flat + k) % total).wait_recv()

    crps[...] = jnp.sum(cr_rx[...], axis=0)

    out_copy.wait_recv()
    gout[...] = (gout_tx[...].astype(jnp.float32) + gout_rx[...].astype(jnp.float32)).T

    @pl.loop(1, total)
    def collect(k):
        fin_copy(flat, (flat + k) % total).wait_recv()

    for owner in range(n):
        gin[:, owner * cw : (owner + 1) * cw] = gin_rx[owner].astype(jnp.float32) + gin_rx[n + owner].astype(jnp.float32)

    @pl.loop(0, tiles)
    def settle(tile):
        back, here = home(tile)
        back.wait_send()
        here.wait()
        arrival(tile).wait_recv()

    @pl.loop(0, chips - 1)
    def settle_ring(step):
        for which in range(2):
            ring_sum(which, step).wait_send()

    @pl.loop(0, chips)
    def settle_pair(step):
        for which in range(2):
            pair_sum(which, step).wait_send()

    out_copy.wait_send()

    @pl.loop(1, total)
    def settle_rest(k):
        to = (flat + k) % total
        cr_copy(to, flat).wait_send()
        fin_copy(to, flat).wait_send()


def fits(rows, width, hidden, n):
    return (
        n >= 4
        and n % 4 == 0
        and hidden % n == 0
        and (hidden // n) % 128 == 0
        and width % n == 0
        and (width // n) % 16 == 0
        and width % 128 == 0
        and hidden % WIDE == 0
        and rows % (2 * TILE) == 0
        and rows * hidden <= 2048 * 2048
        and width * hidden <= 512 * 2048
    )


def fused(latents, noise, cond_gain, cond_shift, w_in, b_in, w_out, target):
    block = latents[0]
    rows, width = block.shape
    n = lax.axis_size("fsdp")
    hidden = w_in.shape[1]
    half = rows // 2
    chips = n // 2
    tiles = half // TILE
    cw = hidden // n
    rin, rout = w_in.shape[0], w_out.shape[0]
    exact = functools.partial(jnp.dot, precision=lax.Precision.HIGHEST, preferred_element_type=jnp.float32)
    gs = jnp.concatenate([1.0 + exact(noise, cond_gain), exact(noise, cond_shift), jnp.zeros((6, width), jnp.float32)])
    bf, f32 = jnp.bfloat16, jnp.float32
    vmem = pl.BlockSpec(memory_space=pltpu.VMEM)
    anywhere = pl.BlockSpec(memory_space=pl.ANY)
    dma = pltpu.SemaphoreType.DMA
    prediction, grad_in, grad_out, parts = pl.pallas_call(
        functools.partial(fused_kernel, n),
        out_shape=(
            jax.ShapeDtypeStruct((rows, width), bf),
            jax.ShapeDtypeStruct((rin, hidden), f32),
            jax.ShapeDtypeStruct((rout, width), f32),
            jax.ShapeDtypeStruct((8, 128), f32),
        ),
        in_specs=[vmem, anywhere, vmem, vmem, vmem, anywhere],
        out_specs=(anywhere, vmem, vmem, vmem),
        scratch_shapes=[
            pltpu.VMEM((width, hidden), bf),
            pltpu.VMEM((hidden, width), bf),
            pltpu.VMEM((2, half, width), bf),
            pltpu.VMEM((half, width), bf),
            pltpu.VMEM((2, 8, width), f32),
            pltpu.VMEM((2, half, width), bf),
            pltpu.VMEM((width, rows), bf),
            pltpu.VMEM((2 * TILE, width), bf),
            pltpu.VMEM((rows, hidden), bf),
            pltpu.VMEM((2 * TILE, hidden), f32),
            pltpu.VMEM((2 * TILE, width), bf),
            pltpu.VMEM((width, rows), bf),
            pltpu.VMEM((rows, hidden), bf),
            pltpu.VMEM((8, width), f32),
            pltpu.VMEM((chips, 2, width, cw), bf),
            pltpu.VMEM((chips, 2, width, cw), bf),
            pltpu.VMEM((chips - 1, 2, width, cw), bf),
            pltpu.VMEM((chips - 1, 2, width, cw), bf),
            pltpu.VMEM((chips, 2, width, cw), f32),
            pltpu.VMEM((width, cw), bf),
            pltpu.VMEM((width, cw), bf),
            pltpu.VMEM((2 * n, rin, cw), bf),
            pltpu.VMEM((width, cw), bf),
            pltpu.VMEM((8, 128), f32),
            pltpu.VMEM((2 * n, 8, 128), f32),
            dma((2, chips)),
            dma((2, chips)),
            dma((2, chips)),
            dma((2, chips)),
            dma((2,)),
            dma((2,)),
            dma((2,)),
            dma((tiles,)),
            dma((tiles,)),
            dma((tiles,)),
            dma((chips, 2)),
            dma((chips, 2)),
            dma((chips, 2)),
            dma((chips, 2)),
            dma((2 * n,)),
            dma((2 * n,)),
            dma,
            dma,
            dma((2 * n,)),
            dma((2 * n,)),
        ],
        compiler_params=pltpu.CompilerParams(
            collective_id=0, has_side_effects=True, vmem_limit_bytes=60 * 1024 * 1024
        ),
    )(gs, block, b_in[None, :], w_in, w_out, target)
    crps_mean = jnp.sum(parts) / jnp.float32(2 * rows * n * width)
    return (prediction[None], grad_in, grad_out, crps_mean)


def on_device(latents, noise, cond_gain, cond_shift, w_in, b_in, w_out, target):
    n = lax.axis_size("fsdp")
    form = fused if fits(latents.shape[1], latents.shape[2], w_in.shape[1], n) else general
    return form(latents, noise, cond_gain, cond_shift, w_in, b_in, w_out, target)


def solution(mesh):
    placed = (
        P("member", "fsdp", None),
        P("member", None),
        P(),
        P(),
        P("fsdp", None),
        P(),
        P("fsdp", None),
        P("fsdp", None),
    )
    return jax.shard_map(
        on_device,
        mesh=mesh,
        in_specs=placed,
        out_specs=(P("member", "fsdp", None), P("fsdp", None), P("fsdp", None), P()),
        check_vma=False,
    )
```

```python
import functools

import jax
import jax.numpy as jnp
from jax import lax
from jax.experimental import pallas as pl
from jax.experimental.pallas import tpu as pltpu
from jax.sharding import PartitionSpec as P

COEF = 0.7978845608
CUBIC = 0.044715


def swapped(block, axis, apart):
    count = lax.axis_size(axis)
    route = []
    for low in range(count):
        high = low | 1 << apart
        if high != low and high < count:
            route += [(low, high), (high, low)]
    return lax.ppermute(block, axis, route)


def gelu_value(v):
    return 0.5 * v * (1.0 + jnp.tanh(COEF * (v + CUBIC * v * v * v)))


def gelu_slope(v):
    u = jnp.tanh(COEF * (v + CUBIC * v * v * v))
    return 0.5 * (1.0 + u) + 0.5 * v * (1.0 - u * u) * COEF * (1.0 + 3.0 * CUBIC * v * v)


def smooth(d):
    return jnp.sqrt(d * d + 0.0625)


def general(latents, noise, cond_gain, cond_shift, w_in, b_in, w_out, target):
    block = latents[0]
    noise_row = noise[0]
    rows = block.shape[0]
    width = block.shape[1]
    groups = lax.axis_size("fsdp")
    nodes = rows * groups
    gain = (
        1.0
        + jnp.dot(
            noise_row[None, :],
            cond_gain,
            precision=lax.Precision.HIGHEST,
            preferred_element_type=jnp.float32,
        )[0]
    )
    shift = jnp.dot(
        noise_row[None, :],
        cond_shift,
        precision=lax.Precision.HIGHEST,
        preferred_element_type=jnp.float32,
    )[0]
    values = block.astype(jnp.float32)
    center = jnp.mean(values, axis=1, keepdims=True)
    spread = jnp.mean((values - center) ** 2, axis=1, keepdims=True)
    normed = ((values - center) / jnp.sqrt(spread + 0.25) * gain + shift).astype(jnp.bfloat16)
    columns = normed
    pre = (
        jnp.dot(
            columns,
            lax.all_gather(w_in, "fsdp", axis=0, tiled=True),
            preferred_element_type=jnp.float32,
        )
        + b_in
    )
    act = gelu_value(pre).astype(jnp.bfloat16)
    columns = act
    output = values + jnp.dot(
        columns,
        lax.all_gather(w_out, "fsdp", axis=0, tiled=True),
        preferred_element_type=jnp.float32,
    )
    prediction = output.astype(jnp.bfloat16)
    partner = swapped(prediction, "member", 0)
    mine = prediction.astype(jnp.float32)
    near = mine - target.astype(jnp.float32)
    apart = mine - partner.astype(jnp.float32)
    local_sum = jnp.sum(0.5 * smooth(near) - 0.25 * smooth(apart))
    crps_mean = lax.psum(local_sum, ("member", "fsdp")) / jnp.float32(2 * nodes * width)
    scale = 1.0 / jnp.sqrt(jnp.float32(2 * nodes))
    dpred = ((0.5 * near / smooth(near) - 0.5 * apart / smooth(apart)) * scale).astype(jnp.bfloat16)
    across = (((1,), (1,)), ((), ()))
    dact = lax.dot_general(
        dpred,
        lax.all_gather(w_out, "fsdp", axis=0, tiled=True),
        across,
        preferred_element_type=jnp.float32,
    )
    dpre = (dact * gelu_slope(pre)).astype(jnp.bfloat16)
    contract = (((0,), (0,)), ((), ()))
    columns = normed
    shard_in = lax.psum_scatter(
        lax.dot_general(columns, dpre, contract, preferred_element_type=jnp.float32),
        "fsdp",
        scatter_dimension=0,
        tiled=True,
    )
    columns = act
    shard_out = lax.psum_scatter(
        lax.dot_general(columns, dpred, contract, preferred_element_type=jnp.float32),
        "fsdp",
        scatter_dimension=0,
        tiled=True,
    )
    grad_in, grad_out = lax.psum((shard_in, shard_out), "member")
    return (prediction[None], grad_in, grad_out, crps_mean)


TILE = 256
WIDE = 512
MESH = pl.DeviceIdType.MESH


def fused_kernel(
    n, noise, cond_gain, cond_shift, lat, b_in, w_in, w_out, target,
    pred, gin, gout, crps,
    win_s, wout_s, x_s, t_s, gs_in, gs_s, p_s, norm_t, norm_s, act_s, slope_s, dp_s, dp_t, dpre_s, cr_s,
    pair_tx, pair_rx, ring_tx, ring_rx, mine_s, gin_tx, gout_tx, gin_rx, gout_rx, cr_tx, cr_rx,
    g_send, g_recv, q_send, q_recv, l_send, l_recv, local_sem, p_send, p_recv, o_sem,
    pair_ss, pair_rs, ring_ss, ring_rs, fin_ss, fin_rs, out_ss, out_rs, cr_ss, cr_rs,
):
    m = lax.axis_index("member")
    f = lax.axis_index("fsdp")
    chips = n // 2
    core = f % 2
    chip = f // 2
    turn = 1 - 2 * core

    def chip_at(place):
        low = place < chips // 2
        return jnp.where(low, 2 * place, 2 * (chips - 1 - place) + 1)

    position = jnp.where(chip % 2 == 0, chip // 2, chips - 1 - chip // 2)

    def place(offset):
        return (position + turn * offset + 2 * chips) % chips

    neighbours = ((m, 2 * chip_at(place(1)) + core), (m, 2 * chip_at(place(-1)) + core))
    hops = (chips // 2, chips - 1 - chips // 2)
    signs = (1, -1)
    twin = (m, 2 * chip + 1 - core)
    partner = (1 - m, f)
    flat = m * n + f
    total = 2 * n

    def device(index):
        return (index // n, index % n)

    barrier = pltpu.get_barrier_semaphore()

    @pl.loop(1, total)
    def greet(k):
        pl.semaphore_signal(barrier, inc=1, device_id=device((flat + k) % total), device_id_type=MESH)

    line = jnp.broadcast_to(noise[...], (8, noise.shape[1]))
    for at, (base, table) in enumerate(((1.0, cond_gain), (0.0, cond_shift))):
        product = jnp.dot(line, table[...], precision=lax.Precision.HIGHEST, preferred_element_type=jnp.float32)
        gs_in[at] = base + product
    pl.semaphore_wait(barrier, total - 1)

    def remote(src, dst, send, recv, to):
        return pltpu.make_async_remote_copy(
            src_ref=src, dst_ref=dst, send_sem=send, recv_sem=recv, device_id=to, device_id_type=MESH
        )

    half = x_s.shape[1]
    width = x_s.shape[2]
    hidden = win_s.shape[1]
    rin = w_in.shape[0]
    rout = w_out.shape[0]
    mine_from = pl.multiple_of(m * half, half)
    other_from = pl.multiple_of((1 - m) * half, half)

    def slot(which, owner):
        if which == 0:
            return win_s.at[pl.ds(pl.multiple_of(owner * rin, rin), rin)]
        return wout_s.at[pl.ds(pl.multiple_of(owner * rout, rout), rout)]

    def ring_copy(which, way, step, src, owner):
        return remote(
            src, slot(which, owner), g_send.at[which, way, step], g_recv.at[which, way, step], neighbours[way]
        )

    def pair_copy(which, way, step, src, owner):
        return remote(src, slot(which, owner), q_send.at[which, way, step], q_recv.at[which, way, step], twin)

    shards = (w_in, w_out)
    for which in range(2):
        for way in range(2):
            ring_copy(which, way, 0, shards[which], f).start()
    swap = remote(lat.at[pl.ds(other_from, half)], x_s.at[0], l_send.at[0], l_recv.at[0], partner)
    swap.start()
    gs_swap = remote(gs_in, gs_s.at[0], l_send.at[1], l_recv.at[1], partner)
    gs_swap.start()
    for which in range(2):
        pair_copy(which, 0, 0, shards[which], f).start()
    keep = pltpu.make_async_copy(lat.at[pl.ds(mine_from, half)], x_s.at[1], local_sem.at[0])
    keep.start()
    goal = pltpu.make_async_copy(target.at[pl.ds(mine_from, half)], t_s, local_sem.at[1])
    goal.start()
    gs_s[1] = gs_in[...]
    cr_s[...] = jnp.zeros_like(cr_s)
    win_s[pl.ds(pl.multiple_of(f * rin, rin), rin), :] = w_in[...]
    wout_s[pl.ds(pl.multiple_of(f * rout, rout), rout), :] = w_out[...]

    passed = []
    for step in range(1, hops[0] + 1):
        for which in range(2):
            for way in range(2):
                if step > hops[way]:
                    continue
                owner = 2 * chip_at(place(-signs[way] * step)) + core
                here = slot(which, owner)
                ring_copy(which, way, step - 1, here, owner).wait_recv()
                if step < hops[way]:
                    onward = ring_copy(which, way, step, here, owner)
                    onward.start()
                    passed.append(onward)
                share = pair_copy(which, way, step, here, owner)
                share.start()
                passed.append(share)
    for which in range(2):
        pair_copy(which, 0, 0, shards[which], 2 * chip + 1 - core).wait_recv()
        for way in range(2):
            for step in range(1, hops[way] + 1):
                owner = 2 * chip_at(place(signs[way] * step)) + 1 - core
                pair_copy(which, way, step, slot(which, owner), owner).wait_recv()
    for which in range(2):
        for way in range(2):
            passed.append(ring_copy(which, way, 0, shards[which], f))
        passed.append(pair_copy(which, 0, 0, shards[which], f))
    for sent in passed:
        sent.wait_send()
    keep.wait()
    goal.wait()
    gs_swap.wait()
    swap.wait()

    tiles = half // TILE
    scale = (1.0 / (2.0 * n * 2 * half) ** 0.5)

    def home(tile):
        start = pl.multiple_of(tile * TILE, TILE)
        there = pl.multiple_of(m * half + tile * TILE, TILE)
        back = remote(p_s.at[0, pl.ds(start, TILE)], pred.at[pl.ds(there, TILE)], p_send.at[tile], p_recv.at[tile], partner)
        here = pltpu.make_async_copy(p_s.at[1, pl.ds(start, TILE)], pred.at[pl.ds(there, TILE)], o_sem.at[tile])
        return back, here

    def arrival(tile):
        start = pl.multiple_of(tile * TILE, TILE)
        there = pl.multiple_of((1 - m) * half + tile * TILE, TILE)
        return remote(p_s.at[0, pl.ds(start, TILE)], pred.at[pl.ds(there, TILE)], p_send.at[tile], p_recv.at[tile], partner)

    @pl.loop(0, tiles)
    def nodes(tile):
        start = pl.multiple_of(tile * TILE, TILE)
        base = pl.multiple_of(tile * 2 * TILE, 2 * TILE)
        rows = pl.ds(base, 2 * TILE)
        for side in range(2):
            values = x_s[side, pl.ds(start, TILE), :].astype(jnp.float32)
            center = jnp.mean(values, axis=1, keepdims=True)
            moved = values - center
            spread = jnp.mean(moved * moved, axis=1, keepdims=True)
            normed = moved * lax.rsqrt(spread + 0.25) * gs_s[side, 0, 0:1, :] + gs_s[side, 1, 0:1, :]
            normed = normed.astype(jnp.bfloat16)
            norm_s[side * TILE : (side + 1) * TILE, :] = normed
        norm_t[:, rows] = norm_s[...].T
        for j in range(hidden // WIDE):
            cols = slice(j * WIDE, (j + 1) * WIDE)
            v = jnp.dot(norm_s[...], win_s[:, cols], preferred_element_type=jnp.float32) + b_in[:, cols]
            square = v * v
            u = jnp.tanh(COEF * (v + CUBIC * square * v))
            gate = 0.5 * (1.0 + u)
            act_s[rows, cols] = (v * gate).astype(jnp.bfloat16)
            slope_s[:, cols] = gate + (0.5 * COEF) * v * (1.0 - u * u) * (1.0 + 3.0 * CUBIC * square)
        out = jnp.dot(act_s[rows, :], wout_s[...], preferred_element_type=jnp.float32)
        guess = []
        for side in range(2):
            value = x_s[side, pl.ds(start, TILE), :].astype(jnp.float32) + out[side * TILE : (side + 1) * TILE]
            value = value.astype(jnp.bfloat16)
            p_s[side, pl.ds(start, TILE), :] = value
            guess.append(value.astype(jnp.float32))
        goal_tile = t_s[pl.ds(start, TILE), :].astype(jnp.float32)
        slopes = []
        value_sum = None
        for d, weight in ((guess[0] - goal_tile, 0.5), (guess[1] - goal_tile, 0.5), (guess[0] - guess[1], -0.5)):
            q = d * d + 0.0625
            r = lax.rsqrt(q)
            slopes.append(0.5 * d * r)
            term = weight * (q * r)
            value_sum = term if value_sum is None else value_sum + term
        cr_s[...] += jnp.sum(value_sum.reshape(TILE // 8, 8, width), axis=0)
        dp_s[:TILE, :] = ((slopes[0] - slopes[2]) * scale).astype(jnp.bfloat16)
        dp_s[TILE:, :] = ((slopes[1] + slopes[2]) * scale).astype(jnp.bfloat16)
        dp_t[:, rows] = dp_s[...].T
        for j in range(hidden // WIDE):
            cols = slice(j * WIDE, (j + 1) * WIDE)
            dact = lax.dot_general(
                dp_s[...], wout_s[cols, :], (((1,), (1,)), ((), ())), preferred_element_type=jnp.float32
            )
            dpre_s[rows, cols] = (dact * slope_s[:, cols]).astype(jnp.bfloat16)
        back, here = home(tile)
        back.start()
        here.start()

    part = cr_s[:, 0:128]
    for j in range(1, width // 128):
        part = part + cr_s[:, j * 128 : (j + 1) * 128]
    cr_tx[...] = part
    cr_rx[flat] = part

    def cr_copy(to, source):
        return remote(cr_tx, cr_rx.at[source], cr_ss.at[to], cr_rs.at[source], device(to))

    cw = hidden // n

    def columns(owner):
        return pl.ds(pl.multiple_of(owner * cw, cw), cw)

    def pair_sum(way, step, which):
        at = (way, step, which)
        return remote(pair_tx.at[at], pair_rx.at[at], pair_ss.at[at], pair_rs.at[at], twin)

    def ring_sum(way, step, which):
        at = (way, step, which)
        return remote(ring_tx.at[at], ring_rx.at[at], ring_ss.at[at], ring_rs.at[at], neighbours[way])

    stages = hops[0]

    def compute(step):
        for way in range(2):
            away = signs[way] * (hops[way] - step)
            own = columns(2 * chip_at(place(away)) + core)
            twins = columns(2 * chip_at(place(-away)) + 1 - core)
            for which, (left, right) in enumerate(((norm_t, dpre_s), (dp_t, act_s))):
                both = jnp.concatenate([right[:, own], right[:, twins]], axis=1)
                product = jnp.dot(left[...], both, preferred_element_type=jnp.float32)
                mine_s[way, step, which] = product[:, :cw]
                pair_tx[way, step, which] = product[:, cw:].astype(jnp.bfloat16)
        for way in range(2):
            for which in range(2):
                pair_sum(way, step, which).start()

    def finish(step, first=False, last=False):
        for way in range(2):
            for which in range(2):
                pair_sum(way, step, which).wait_recv()
                value = mine_s[way, step, which] + pair_rx[way, step, which].astype(jnp.float32)
                if not first:
                    ring_sum(way, step - 1, which).wait_recv()
                    value = value + ring_rx[way, step - 1, which].astype(jnp.float32)
                if last and way == 1:
                    ring_sum(0, step, which).wait_recv()
                    value = value + ring_rx[0, step, which].astype(jnp.float32)
                value = value.astype(jnp.bfloat16)
                if not last or way == 0:
                    ring_tx[way, step, which] = value
                    ring_sum(way, step, which).start()
                elif which == 0:
                    gin_tx[...] = value
                else:
                    gout_tx[...] = value

    compute(0)
    compute(1)
    finish(0, first=True)

    @pl.loop(1, stages - 1)
    def steps(step):
        compute(step + 1)
        finish(step)

    @pl.loop(1, total)
    def tell(k):
        cr_copy((flat + k) % total, flat).start()

    finish(stages - 1, last=True)

    def fin_copy(to, source):
        target_rows = pl.ds(pl.multiple_of((to % n) * rin, rin), rin)
        return remote(gin_tx.at[target_rows], gin_rx.at[source], fin_ss.at[to], fin_rs.at[source], device(to))

    out_copy = remote(gout_tx, gout_rx, out_ss, out_rs, partner)
    out_copy.start()

    @pl.loop(1, total)
    def scatter(k):
        fin_copy((flat + k) % total, flat).start()

    gin_rx[flat] = gin_tx[pl.ds(pl.multiple_of(f * rin, rin), rin), :]

    @pl.loop(1, total)
    def heard(k):
        cr_copy(flat, (flat + k) % total).wait_recv()

    crps[0, 0] = jnp.sum(jnp.sum(cr_rx[...], axis=0)) / jnp.float32(4 * n * half * width)

    out_copy.wait_recv()
    gout[...] = (gout_tx[...].astype(jnp.float32) + gout_rx[...].astype(jnp.float32)).T

    @pl.loop(1, total)
    def collect(k):
        fin_copy(flat, (flat + k) % total).wait_recv()

    for owner in range(n):
        gin[:, owner * cw : (owner + 1) * cw] = gin_rx[owner].astype(jnp.float32) + gin_rx[n + owner].astype(jnp.float32)

    @pl.loop(0, tiles)
    def settle(tile):
        back, here = home(tile)
        back.wait_send()
        here.wait()
        arrival(tile).wait_recv()

    @pl.loop(0, stages)
    def settle_pair(step):
        for way in range(2):
            for which in range(2):
                pair_sum(way, step, which).wait_send()

    for way in range(2):

        @pl.loop(0, hops[way])
        def settle_ring(step):
            for which in range(2):
                ring_sum(way, step, which).wait_send()

    out_copy.wait_send()

    @pl.loop(1, total)
    def settle_rest(k):
        to = (flat + k) % total
        cr_copy(to, flat).wait_send()
        fin_copy(to, flat).wait_send()


def fits(rows, width, hidden, n):
    return (
        n >= 4
        and n % 4 == 0
        and hidden % n == 0
        and (hidden // n) % 128 == 0
        and width % n == 0
        and (width // n) % 16 == 0
        and width % 128 == 0
        and hidden % WIDE == 0
        and rows % (2 * TILE) == 0
        and rows * hidden <= 2048 * 2048
        and width * hidden <= 512 * 2048
    )


def fused(latents, noise, cond_gain, cond_shift, w_in, b_in, w_out, target):
    block = latents[0]
    rows, width = block.shape
    n = lax.axis_size("fsdp")
    hidden = w_in.shape[1]
    half = rows // 2
    chips = n // 2
    tiles = half // TILE
    cw = hidden // n
    stages = chips // 2
    rin, rout = w_in.shape[0], w_out.shape[0]
    bf, f32 = jnp.bfloat16, jnp.float32
    vmem = pl.BlockSpec(memory_space=pltpu.VMEM)
    anywhere = pl.BlockSpec(memory_space=pl.ANY)
    dma = pltpu.SemaphoreType.DMA
    prediction, grad_in, grad_out, parts = pl.pallas_call(
        functools.partial(fused_kernel, n),
        out_shape=(
            jax.ShapeDtypeStruct((rows, width), bf),
            jax.ShapeDtypeStruct((rin, hidden), f32),
            jax.ShapeDtypeStruct((rout, width), f32),
            jax.ShapeDtypeStruct((1, 1), f32),
        ),
        in_specs=[vmem, vmem, vmem, anywhere, vmem, vmem, vmem, anywhere],
        out_specs=(anywhere, vmem, vmem, pl.BlockSpec(memory_space=pltpu.SMEM)),
        scratch_shapes=[
            pltpu.VMEM((width, hidden), bf),
            pltpu.VMEM((hidden, width), bf),
            pltpu.VMEM((2, half, width), bf),
            pltpu.VMEM((half, width), bf),
            pltpu.VMEM((2, 8, width), f32),
            pltpu.VMEM((2, 2, 8, width), f32),
            pltpu.VMEM((2, half, width), bf),
            pltpu.VMEM((width, rows), bf),
            pltpu.VMEM((2 * TILE, width), bf),
            pltpu.VMEM((rows, hidden), bf),
            pltpu.VMEM((2 * TILE, hidden), f32),
            pltpu.VMEM((2 * TILE, width), bf),
            pltpu.VMEM((width, rows), bf),
            pltpu.VMEM((rows, hidden), bf),
            pltpu.VMEM((8, width), f32),
            pltpu.VMEM((2, stages, 2, width, cw), bf),
            pltpu.VMEM((2, stages, 2, width, cw), bf),
            pltpu.VMEM((2, stages, 2, width, cw), bf),
            pltpu.VMEM((2, stages, 2, width, cw), bf),
            pltpu.VMEM((2, stages, 2, width, cw), f32),
            pltpu.VMEM((width, cw), bf),
            pltpu.VMEM((width, cw), bf),
            pltpu.VMEM((2 * n, rin, cw), bf),
            pltpu.VMEM((width, cw), bf),
            pltpu.VMEM((8, 128), f32),
            pltpu.VMEM((2 * n, 8, 128), f32),
            dma((2, 2, stages + 1)),
            dma((2, 2, stages + 1)),
            dma((2, 2, stages + 1)),
            dma((2, 2, stages + 1)),
            dma((2,)),
            dma((2,)),
            dma((2,)),
            dma((tiles,)),
            dma((tiles,)),
            dma((tiles,)),
            dma((2, stages, 2)),
            dma((2, stages, 2)),
            dma((2, stages, 2)),
            dma((2, stages, 2)),
            dma((2 * n,)),
            dma((2 * n,)),
            dma,
            dma,
            dma((2 * n,)),
            dma((2 * n,)),
        ],
        compiler_params=pltpu.CompilerParams(
            collective_id=0, has_side_effects=True, vmem_limit_bytes=60 * 1024 * 1024
        ),
    )(noise, cond_gain, cond_shift, block, b_in[None, :], w_in, w_out, target)
    crps_mean = parts.reshape(())
    return (prediction[None], grad_in, grad_out, crps_mean)


def on_device(latents, noise, cond_gain, cond_shift, w_in, b_in, w_out, target):
    n = lax.axis_size("fsdp")
    form = fused if fits(latents.shape[1], latents.shape[2], w_in.shape[1], n) else general
    return form(latents, noise, cond_gain, cond_shift, w_in, b_in, w_out, target)


def solution(mesh):
    placed = (
        P("member", "fsdp", None),
        P("member", None),
        P(),
        P(),
        P("fsdp", None),
        P(),
        P("fsdp", None),
        P("fsdp", None),
    )
    return jax.shard_map(
        on_device,
        mesh=mesh,
        in_specs=placed,
        out_specs=(P("member", "fsdp", None), P("fsdp", None), P("fsdp", None), P()),
        check_vma=False,
    )
```

```python
import functools

import jax
import jax.numpy as jnp
from jax import lax
from jax.experimental import pallas as pl
from jax.experimental.pallas import tpu as pltpu
from jax.sharding import PartitionSpec as P

COEF = 0.7978845608
CUBIC = 0.044715


def swapped(block, axis, apart):
    count = lax.axis_size(axis)
    route = []
    for low in range(count):
        high = low | 1 << apart
        if high != low and high < count:
            route += [(low, high), (high, low)]
    return lax.ppermute(block, axis, route)


def gelu_value(v):
    return 0.5 * v * (1.0 + jnp.tanh(COEF * (v + CUBIC * v * v * v)))


def gelu_slope(v):
    u = jnp.tanh(COEF * (v + CUBIC * v * v * v))
    return 0.5 * (1.0 + u) + 0.5 * v * (1.0 - u * u) * COEF * (1.0 + 3.0 * CUBIC * v * v)


def smooth(d):
    return jnp.sqrt(d * d + 0.0625)


def general(latents, noise, cond_gain, cond_shift, w_in, b_in, w_out, target):
    block = latents[0]
    noise_row = noise[0]
    rows = block.shape[0]
    width = block.shape[1]
    groups = lax.axis_size("fsdp")
    nodes = rows * groups
    gain = (
        1.0
        + jnp.dot(
            noise_row[None, :],
            cond_gain,
            precision=lax.Precision.HIGHEST,
            preferred_element_type=jnp.float32,
        )[0]
    )
    shift = jnp.dot(
        noise_row[None, :],
        cond_shift,
        precision=lax.Precision.HIGHEST,
        preferred_element_type=jnp.float32,
    )[0]
    values = block.astype(jnp.float32)
    center = jnp.mean(values, axis=1, keepdims=True)
    spread = jnp.mean((values - center) ** 2, axis=1, keepdims=True)
    normed = ((values - center) / jnp.sqrt(spread + 0.25) * gain + shift).astype(jnp.bfloat16)
    columns = normed
    pre = (
        jnp.dot(
            columns,
            lax.all_gather(w_in, "fsdp", axis=0, tiled=True),
            preferred_element_type=jnp.float32,
        )
        + b_in
    )
    act = gelu_value(pre).astype(jnp.bfloat16)
    columns = act
    output = values + jnp.dot(
        columns,
        lax.all_gather(w_out, "fsdp", axis=0, tiled=True),
        preferred_element_type=jnp.float32,
    )
    prediction = output.astype(jnp.bfloat16)
    partner = swapped(prediction, "member", 0)
    mine = prediction.astype(jnp.float32)
    near = mine - target.astype(jnp.float32)
    apart = mine - partner.astype(jnp.float32)
    local_sum = jnp.sum(0.5 * smooth(near) - 0.25 * smooth(apart))
    crps_mean = lax.psum(local_sum, ("member", "fsdp")) / jnp.float32(2 * nodes * width)
    scale = 1.0 / jnp.sqrt(jnp.float32(2 * nodes))
    dpred = ((0.5 * near / smooth(near) - 0.5 * apart / smooth(apart)) * scale).astype(jnp.bfloat16)
    across = (((1,), (1,)), ((), ()))
    dact = lax.dot_general(
        dpred,
        lax.all_gather(w_out, "fsdp", axis=0, tiled=True),
        across,
        preferred_element_type=jnp.float32,
    )
    dpre = (dact * gelu_slope(pre)).astype(jnp.bfloat16)
    contract = (((0,), (0,)), ((), ()))
    columns = normed
    shard_in = lax.psum_scatter(
        lax.dot_general(columns, dpre, contract, preferred_element_type=jnp.float32),
        "fsdp",
        scatter_dimension=0,
        tiled=True,
    )
    columns = act
    shard_out = lax.psum_scatter(
        lax.dot_general(columns, dpred, contract, preferred_element_type=jnp.float32),
        "fsdp",
        scatter_dimension=0,
        tiled=True,
    )
    grad_in, grad_out = lax.psum((shard_in, shard_out), "member")
    return (prediction[None], grad_in, grad_out, crps_mean)


TILE = 256
WIDE = 512
MESH = pl.DeviceIdType.MESH


def fused_kernel(
    n, noise, cond_gain, cond_shift, lat, b_in, w_in, w_out, target,
    pred, gin, gout, crps,
    win_s, wout_s, x_s, t_s, gs_in, gs_s, p_s, norm_t, norm_s, act_s, dp_s, dp_t, dpre_s, cr_s,
    pair_tx, pair_rx, ring_tx, ring_rx, mine_s, gin_tx, gout_tx, gin_rx, gout_rx, cr_tx, cr_rx,
    g_send, g_recv, q_send, q_recv, l_send, l_recv, local_sem, p_send, p_recv, o_sem,
    pair_ss, pair_rs, ring_ss, ring_rs, fin_ss, fin_rs, out_ss, out_rs, cr_ss, cr_rs,
):
    m = lax.axis_index("member")
    f = lax.axis_index("fsdp")
    chips = n // 2
    core = f % 2
    chip = f // 2
    turn = 1 - 2 * core

    def chip_at(place):
        low = place < chips // 2
        return jnp.where(low, 2 * place, 2 * (chips - 1 - place) + 1)

    position = jnp.where(chip % 2 == 0, chip // 2, chips - 1 - chip // 2)

    def place(offset):
        return (position + turn * offset + 2 * chips) % chips

    neighbours = ((m, 2 * chip_at(place(1)) + core), (m, 2 * chip_at(place(-1)) + core))
    hops = (chips // 2, chips - 1 - chips // 2)
    signs = (1, -1)
    twin = (m, 2 * chip + 1 - core)
    partner = (1 - m, f)
    flat = m * n + f
    total = 2 * n

    def device(index):
        return (index // n, index % n)

    barrier = pltpu.get_barrier_semaphore()

    @pl.loop(1, total)
    def greet(k):
        pl.semaphore_signal(barrier, inc=1, device_id=device((flat + k) % total), device_id_type=MESH)

    line = jnp.broadcast_to(noise[...], (8, noise.shape[1]))
    for at, (base, table) in enumerate(((1.0, cond_gain), (0.0, cond_shift))):
        product = jnp.dot(line, table[...], precision=lax.Precision.HIGHEST, preferred_element_type=jnp.float32)
        gs_in[at] = base + product
    pl.semaphore_wait(barrier, total - 1)

    def remote(src, dst, send, recv, to):
        return pltpu.make_async_remote_copy(
            src_ref=src, dst_ref=dst, send_sem=send, recv_sem=recv, device_id=to, device_id_type=MESH
        )

    half = x_s.shape[1]
    width = x_s.shape[2]
    hidden = win_s.shape[1]
    rin = w_in.shape[0]
    rout = w_out.shape[0]
    mine_from = pl.multiple_of(m * half, half)
    other_from = pl.multiple_of((1 - m) * half, half)

    def slot(which, owner):
        if which == 0:
            return win_s.at[pl.ds(pl.multiple_of(owner * rin, rin), rin)]
        return wout_s.at[pl.ds(pl.multiple_of(owner * rout, rout), rout)]

    def ring_copy(which, way, step, src, owner):
        return remote(
            src, slot(which, owner), g_send.at[which, way, step], g_recv.at[which, way, step], neighbours[way]
        )

    def pair_copy(which, way, step, src, owner):
        return remote(src, slot(which, owner), q_send.at[which, way, step], q_recv.at[which, way, step], twin)

    shards = (w_in, w_out)
    for which in range(2):
        for way in range(2):
            ring_copy(which, way, 0, shards[which], f).start()
    swap = remote(lat.at[pl.ds(other_from, half)], x_s.at[0], l_send.at[0], l_recv.at[0], partner)
    swap.start()
    gs_swap = remote(gs_in, gs_s.at[0], l_send.at[1], l_recv.at[1], partner)
    gs_swap.start()
    for which in range(2):
        pair_copy(which, 0, 0, shards[which], f).start()
    keep = pltpu.make_async_copy(lat.at[pl.ds(mine_from, half)], x_s.at[1], local_sem.at[0])
    keep.start()
    goal = pltpu.make_async_copy(target.at[pl.ds(mine_from, half)], t_s, local_sem.at[1])
    goal.start()
    gs_s[1] = gs_in[...]
    cr_s[...] = jnp.zeros_like(cr_s)
    win_s[pl.ds(pl.multiple_of(f * rin, rin), rin), :] = w_in[...]
    wout_s[pl.ds(pl.multiple_of(f * rout, rout), rout), :] = w_out[...]

    passed = []

    def forward(which, way, step):
        owner = 2 * chip_at(place(-signs[way] * step)) + core
        here = slot(which, owner)
        ring_copy(which, way, step - 1, here, owner).wait_recv()
        if step < hops[way]:
            onward = ring_copy(which, way, step, here, owner)
            onward.start()
            passed.append(onward)
        share = pair_copy(which, way, step, here, owner)
        share.start()
        passed.append(share)

    def shared(which):
        pair_copy(which, 0, 0, shards[which], 2 * chip + 1 - core).wait_recv()
        for way in range(2):
            for step in range(1, hops[way] + 1):
                owner = 2 * chip_at(place(signs[way] * step)) + 1 - core
                pair_copy(which, way, step, slot(which, owner), owner).wait_recv()

    def hidden_units(side, tile):
        start = pl.multiple_of(tile * WIDE, WIDE)
        rows = pl.ds(pl.multiple_of(side * half + start, WIDE), WIDE)
        values = x_s[side, pl.ds(start, WIDE), :].astype(jnp.float32)
        center = jnp.mean(values, axis=1, keepdims=True)
        moved = values - center
        spread = jnp.mean(moved * moved, axis=1, keepdims=True)
        normed = moved * lax.rsqrt(spread + 0.25) * gs_s[side, 0, 0:1, :] + gs_s[side, 1, 0:1, :]
        norm_s[...] = normed.astype(jnp.bfloat16)
        norm_t[:, rows] = norm_s[...].T
        for j in range(hidden // WIDE):
            cols = slice(j * WIDE, (j + 1) * WIDE)
            v = jnp.dot(norm_s[...], win_s[:, cols], preferred_element_type=jnp.float32) + b_in[:, cols]
            square = v * v
            u = jnp.tanh(COEF * (v + CUBIC * square * v))
            gate = 0.5 * (1.0 + u)
            act_s[rows, cols] = (v * gate).astype(jnp.bfloat16)
            slope = gate + (0.5 * COEF) * v * (1.0 - u * u) * (1.0 + 3.0 * CUBIC * square)
            dpre_s[rows, cols] = slope.astype(jnp.bfloat16)

    for step in range(1, hops[0]):
        for which in range(2):
            for way in range(2):
                forward(which, way, step)
    forward(0, 0, hops[0])
    keep.wait()
    shared(0)

    @pl.loop(0, half // WIDE)
    def own_side(tile):
        hidden_units(1, tile)

    forward(1, 0, hops[0])
    gs_swap.wait()
    swap.wait()

    @pl.loop(0, half // WIDE)
    def other_side(tile):
        hidden_units(0, tile)

    shared(1)
    for which in range(2):
        for way in range(2):
            passed.append(ring_copy(which, way, 0, shards[which], f))
        passed.append(pair_copy(which, 0, 0, shards[which], f))
    for sent in passed:
        sent.wait_send()
    goal.wait()

    tiles = half // TILE
    scale = (1.0 / (2.0 * n * 2 * half) ** 0.5)

    def home(tile):
        start = pl.multiple_of(tile * TILE, TILE)
        there = pl.multiple_of(m * half + tile * TILE, TILE)
        back = remote(p_s.at[0, pl.ds(start, TILE)], pred.at[pl.ds(there, TILE)], p_send.at[tile], p_recv.at[tile], partner)
        here = pltpu.make_async_copy(p_s.at[1, pl.ds(start, TILE)], pred.at[pl.ds(there, TILE)], o_sem.at[tile])
        return back, here

    def arrival(tile):
        start = pl.multiple_of(tile * TILE, TILE)
        there = pl.multiple_of((1 - m) * half + tile * TILE, TILE)
        return remote(p_s.at[0, pl.ds(start, TILE)], pred.at[pl.ds(there, TILE)], p_send.at[tile], p_recv.at[tile], partner)

    @pl.loop(0, tiles)
    def nodes(tile):
        start = pl.multiple_of(tile * TILE, TILE)
        parts = (pl.ds(start, TILE), pl.ds(pl.multiple_of(half + start, TILE), TILE))
        acts = jnp.concatenate([act_s[rows, :] for rows in parts], axis=0)
        out = jnp.dot(acts, wout_s[...], preferred_element_type=jnp.float32)
        guess = []
        for side in range(2):
            value = x_s[side, pl.ds(start, TILE), :].astype(jnp.float32) + out[side * TILE : (side + 1) * TILE]
            value = value.astype(jnp.bfloat16)
            p_s[side, pl.ds(start, TILE), :] = value
            guess.append(value.astype(jnp.float32))
        goal_tile = t_s[pl.ds(start, TILE), :].astype(jnp.float32)
        slopes = []
        value_sum = None
        for d, weight in ((guess[0] - goal_tile, 0.5), (guess[1] - goal_tile, 0.5), (guess[0] - guess[1], -0.5)):
            q = d * d + 0.0625
            r = lax.rsqrt(q)
            slopes.append(0.5 * d * r)
            term = weight * (q * r)
            value_sum = term if value_sum is None else value_sum + term
        cr_s[...] += jnp.sum(value_sum.reshape(TILE // 8, 8, width), axis=0)
        dp_s[:TILE, :] = ((slopes[0] - slopes[2]) * scale).astype(jnp.bfloat16)
        dp_s[TILE:, :] = ((slopes[1] + slopes[2]) * scale).astype(jnp.bfloat16)
        turned = dp_s[...].T
        for side, rows in enumerate(parts):
            dp_t[:, rows] = turned[:, side * TILE : (side + 1) * TILE]
        for j in range(hidden // WIDE):
            cols = slice(j * WIDE, (j + 1) * WIDE)
            dact = lax.dot_general(
                dp_s[...], wout_s[cols, :], (((1,), (1,)), ((), ())), preferred_element_type=jnp.float32
            )
            for side, rows in enumerate(parts):
                piece = dact[side * TILE : (side + 1) * TILE] * dpre_s[rows, cols].astype(jnp.float32)
                dpre_s[rows, cols] = piece.astype(jnp.bfloat16)
        back, here = home(tile)
        back.start()
        here.start()

    part = cr_s[:, 0:128]
    for j in range(1, width // 128):
        part = part + cr_s[:, j * 128 : (j + 1) * 128]
    cr_tx[...] = part
    cr_rx[flat] = part

    def cr_copy(to, source):
        return remote(cr_tx, cr_rx.at[source], cr_ss.at[to], cr_rs.at[source], device(to))

    cw = hidden // n

    def columns(owner):
        return pl.ds(pl.multiple_of(owner * cw, cw), cw)

    def fin_copy(to, source):
        target_rows = pl.ds(pl.multiple_of((to % n) * rin, rin), rin)
        return remote(gin_tx.at[target_rows], gin_rx.at[source], fin_ss.at[to], fin_rs.at[source], device(to))

    out_copy = remote(gout_tx, gout_rx, out_ss, out_rs, partner)

    def pair_sum(way, step, which):
        at = (way, step, which)
        return remote(pair_tx.at[at], pair_rx.at[at], pair_ss.at[at], pair_rs.at[at], twin)

    def ring_sum(way, step, which):
        at = (way, step, which)
        return remote(ring_tx.at[at], ring_rx.at[at], ring_ss.at[at], ring_rs.at[at], neighbours[way])

    stages = hops[0]

    def compute(step):
        for way in range(2):
            away = signs[way] * (hops[way] - step)
            own = columns(2 * chip_at(place(away)) + core)
            twins = columns(2 * chip_at(place(-away)) + 1 - core)
            for which, (left, right) in enumerate(((norm_t, dpre_s), (dp_t, act_s))):
                both = jnp.concatenate([right[:, own], right[:, twins]], axis=1)
                product = jnp.dot(left[...], both, preferred_element_type=jnp.float32)
                mine_s[way, step, which] = product[:, :cw]
                pair_tx[way, step, which] = product[:, cw:].astype(jnp.bfloat16)
        for way in range(2):
            for which in range(2):
                pair_sum(way, step, which).start()

    def finish(step, first=False, last=False):
        for way in range(2):
            for which in range(2):
                pair_sum(way, step, which).wait_recv()
                value = mine_s[way, step, which] + pair_rx[way, step, which].astype(jnp.float32)
                if not first:
                    ring_sum(way, step - 1, which).wait_recv()
                    value = value + ring_rx[way, step - 1, which].astype(jnp.float32)
                if last and way == 1:
                    ring_sum(0, step, which).wait_recv()
                    value = value + ring_rx[0, step, which].astype(jnp.float32)
                value = value.astype(jnp.bfloat16)
                if not last or way == 0:
                    ring_tx[way, step, which] = value
                    ring_sum(way, step, which).start()
                elif which == 0:
                    gin_tx[...] = value

                    @pl.loop(1, total)
                    def scatter(k):
                        fin_copy((flat + k) % total, flat).start()

                else:
                    gout_tx[...] = value
                    out_copy.start()

    compute(0)
    compute(1)
    finish(0, first=True)

    @pl.loop(1, stages - 1)
    def steps(step):
        compute(step + 1)
        finish(step)

    @pl.loop(1, total)
    def tell(k):
        cr_copy((flat + k) % total, flat).start()

    finish(stages - 1, last=True)

    gin_rx[flat] = gin_tx[pl.ds(pl.multiple_of(f * rin, rin), rin), :]

    @pl.loop(1, total)
    def heard(k):
        cr_copy(flat, (flat + k) % total).wait_recv()

    crps[0, 0] = jnp.sum(jnp.sum(cr_rx[...], axis=0)) / jnp.float32(4 * n * half * width)

    out_copy.wait_recv()
    gout[...] = (gout_tx[...].astype(jnp.float32) + gout_rx[...].astype(jnp.float32)).T

    @pl.loop(1, total)
    def collect(k):
        fin_copy(flat, (flat + k) % total).wait_recv()

    for owner in range(n):
        gin[:, owner * cw : (owner + 1) * cw] = gin_rx[owner].astype(jnp.float32) + gin_rx[n + owner].astype(jnp.float32)

    @pl.loop(0, tiles)
    def settle(tile):
        back, here = home(tile)
        back.wait_send()
        here.wait()
        arrival(tile).wait_recv()

    @pl.loop(0, stages)
    def settle_pair(step):
        for way in range(2):
            for which in range(2):
                pair_sum(way, step, which).wait_send()

    for way in range(2):

        @pl.loop(0, hops[way])
        def settle_ring(step):
            for which in range(2):
                ring_sum(way, step, which).wait_send()

    out_copy.wait_send()

    @pl.loop(1, total)
    def settle_rest(k):
        to = (flat + k) % total
        cr_copy(to, flat).wait_send()
        fin_copy(to, flat).wait_send()


def fits(rows, width, hidden, n):
    return (
        n >= 4
        and n % 4 == 0
        and hidden % n == 0
        and (hidden // n) % 128 == 0
        and width % n == 0
        and (width // n) % 16 == 0
        and width % 128 == 0
        and hidden % WIDE == 0
        and rows % (2 * WIDE) == 0
        and rows * hidden <= 2048 * 2048
        and width * hidden <= 512 * 2048
    )


def fused(latents, noise, cond_gain, cond_shift, w_in, b_in, w_out, target):
    block = latents[0]
    rows, width = block.shape
    n = lax.axis_size("fsdp")
    hidden = w_in.shape[1]
    half = rows // 2
    chips = n // 2
    tiles = half // TILE
    cw = hidden // n
    stages = chips // 2
    rin, rout = w_in.shape[0], w_out.shape[0]
    bf, f32 = jnp.bfloat16, jnp.float32
    vmem = pl.BlockSpec(memory_space=pltpu.VMEM)
    anywhere = pl.BlockSpec(memory_space=pl.ANY)
    dma = pltpu.SemaphoreType.DMA
    prediction, grad_in, grad_out, parts = pl.pallas_call(
        functools.partial(fused_kernel, n),
        out_shape=(
            jax.ShapeDtypeStruct((rows, width), bf),
            jax.ShapeDtypeStruct((rin, hidden), f32),
            jax.ShapeDtypeStruct((rout, width), f32),
            jax.ShapeDtypeStruct((1, 1), f32),
        ),
        in_specs=[vmem, vmem, vmem, anywhere, vmem, vmem, vmem, anywhere],
        out_specs=(anywhere, vmem, vmem, pl.BlockSpec(memory_space=pltpu.SMEM)),
        scratch_shapes=[
            pltpu.VMEM((width, hidden), bf),
            pltpu.VMEM((hidden, width), bf),
            pltpu.VMEM((2, half, width), bf),
            pltpu.VMEM((half, width), bf),
            pltpu.VMEM((2, 8, width), f32),
            pltpu.VMEM((2, 2, 8, width), f32),
            pltpu.VMEM((2, half, width), bf),
            pltpu.VMEM((width, rows), bf),
            pltpu.VMEM((WIDE, width), bf),
            pltpu.VMEM((rows, hidden), bf),
            pltpu.VMEM((2 * TILE, width), bf),
            pltpu.VMEM((width, rows), bf),
            pltpu.VMEM((rows, hidden), bf),
            pltpu.VMEM((8, width), f32),
            pltpu.VMEM((2, stages, 2, width, cw), bf),
            pltpu.VMEM((2, stages, 2, width, cw), bf),
            pltpu.VMEM((2, stages, 2, width, cw), bf),
            pltpu.VMEM((2, stages, 2, width, cw), bf),
            pltpu.VMEM((2, stages, 2, width, cw), f32),
            pltpu.VMEM((width, cw), bf),
            pltpu.VMEM((width, cw), bf),
            pltpu.VMEM((2 * n, rin, cw), bf),
            pltpu.VMEM((width, cw), bf),
            pltpu.VMEM((8, 128), f32),
            pltpu.VMEM((2 * n, 8, 128), f32),
            dma((2, 2, stages + 1)),
            dma((2, 2, stages + 1)),
            dma((2, 2, stages + 1)),
            dma((2, 2, stages + 1)),
            dma((2,)),
            dma((2,)),
            dma((2,)),
            dma((tiles,)),
            dma((tiles,)),
            dma((tiles,)),
            dma((2, stages, 2)),
            dma((2, stages, 2)),
            dma((2, stages, 2)),
            dma((2, stages, 2)),
            dma((2 * n,)),
            dma((2 * n,)),
            dma,
            dma,
            dma((2 * n,)),
            dma((2 * n,)),
        ],
        compiler_params=pltpu.CompilerParams(
            collective_id=0, has_side_effects=True, vmem_limit_bytes=60 * 1024 * 1024
        ),
    )(noise, cond_gain, cond_shift, block, b_in[None, :], w_in, w_out, target)
    crps_mean = parts.reshape(())
    return (prediction[None], grad_in, grad_out, crps_mean)


def on_device(latents, noise, cond_gain, cond_shift, w_in, b_in, w_out, target):
    n = lax.axis_size("fsdp")
    form = fused if fits(latents.shape[1], latents.shape[2], w_in.shape[1], n) else general
    return form(latents, noise, cond_gain, cond_shift, w_in, b_in, w_out, target)


def solution(mesh):
    placed = (
        P("member", "fsdp", None),
        P("member", None),
        P(),
        P(),
        P("fsdp", None),
        P(),
        P("fsdp", None),
        P("fsdp", None),
    )
    return jax.shard_map(
        on_device,
        mesh=mesh,
        in_specs=placed,
        out_specs=(P("member", "fsdp", None), P("fsdp", None), P("fsdp", None), P()),
        check_vma=False,
    )
```

```python
import functools

import jax
import jax.numpy as jnp
from jax import lax
from jax.experimental import pallas as pl
from jax.experimental.pallas import tpu as pltpu
from jax.sharding import PartitionSpec as P

COEF = 0.7978845608
CUBIC = 0.044715


def swapped(block, axis, apart):
    count = lax.axis_size(axis)
    route = []
    for low in range(count):
        high = low | 1 << apart
        if high != low and high < count:
            route += [(low, high), (high, low)]
    return lax.ppermute(block, axis, route)


def gelu_value(v):
    return 0.5 * v * (1.0 + jnp.tanh(COEF * (v + CUBIC * v * v * v)))


def gelu_slope(v):
    u = jnp.tanh(COEF * (v + CUBIC * v * v * v))
    return 0.5 * (1.0 + u) + 0.5 * v * (1.0 - u * u) * COEF * (1.0 + 3.0 * CUBIC * v * v)


def smooth(d):
    return jnp.sqrt(d * d + 0.0625)


def general(latents, noise, cond_gain, cond_shift, w_in, b_in, w_out, target):
    block = latents[0]
    noise_row = noise[0]
    rows = block.shape[0]
    width = block.shape[1]
    groups = lax.axis_size("fsdp")
    nodes = rows * groups
    gain = (
        1.0
        + jnp.dot(
            noise_row[None, :],
            cond_gain,
            precision=lax.Precision.HIGHEST,
            preferred_element_type=jnp.float32,
        )[0]
    )
    shift = jnp.dot(
        noise_row[None, :],
        cond_shift,
        precision=lax.Precision.HIGHEST,
        preferred_element_type=jnp.float32,
    )[0]
    values = block.astype(jnp.float32)
    center = jnp.mean(values, axis=1, keepdims=True)
    spread = jnp.mean((values - center) ** 2, axis=1, keepdims=True)
    normed = ((values - center) / jnp.sqrt(spread + 0.25) * gain + shift).astype(jnp.bfloat16)
    columns = normed
    pre = (
        jnp.dot(
            columns,
            lax.all_gather(w_in, "fsdp", axis=0, tiled=True),
            preferred_element_type=jnp.float32,
        )
        + b_in
    )
    act = gelu_value(pre).astype(jnp.bfloat16)
    columns = act
    output = values + jnp.dot(
        columns,
        lax.all_gather(w_out, "fsdp", axis=0, tiled=True),
        preferred_element_type=jnp.float32,
    )
    prediction = output.astype(jnp.bfloat16)
    partner = swapped(prediction, "member", 0)
    mine = prediction.astype(jnp.float32)
    near = mine - target.astype(jnp.float32)
    apart = mine - partner.astype(jnp.float32)
    local_sum = jnp.sum(0.5 * smooth(near) - 0.25 * smooth(apart))
    crps_mean = lax.psum(local_sum, ("member", "fsdp")) / jnp.float32(2 * nodes * width)
    scale = 1.0 / jnp.sqrt(jnp.float32(2 * nodes))
    dpred = ((0.5 * near / smooth(near) - 0.5 * apart / smooth(apart)) * scale).astype(jnp.bfloat16)
    across = (((1,), (1,)), ((), ()))
    dact = lax.dot_general(
        dpred,
        lax.all_gather(w_out, "fsdp", axis=0, tiled=True),
        across,
        preferred_element_type=jnp.float32,
    )
    dpre = (dact * gelu_slope(pre)).astype(jnp.bfloat16)
    contract = (((0,), (0,)), ((), ()))
    columns = normed
    shard_in = lax.psum_scatter(
        lax.dot_general(columns, dpre, contract, preferred_element_type=jnp.float32),
        "fsdp",
        scatter_dimension=0,
        tiled=True,
    )
    columns = act
    shard_out = lax.psum_scatter(
        lax.dot_general(columns, dpred, contract, preferred_element_type=jnp.float32),
        "fsdp",
        scatter_dimension=0,
        tiled=True,
    )
    grad_in, grad_out = lax.psum((shard_in, shard_out), "member")
    return (prediction[None], grad_in, grad_out, crps_mean)


TILE = 256
WIDE = 512
MESH = pl.DeviceIdType.MESH


def fused_kernel(
    n, noise, cond_gain, cond_shift, lat, b_in, w_in, w_out, target,
    pred, gin, gout, crps,
    win_s, wout_s, x_s, t_s, gs_in, gs_s, p_s, norm_t, norm_s, act_s, slope_s, dp_s, dp_t, dpre_s, cr_s,
    pair_tx, pair_rx, ring_tx, ring_rx, mine_s, gin_tx, gout_tx, gin_rx, gout_rx, cr_tx, cr_rx,
    g_send, g_recv, q_send, q_recv, l_send, l_recv, local_sem, p_send, p_recv, o_sem,
    pair_ss, pair_rs, ring_ss, ring_rs, fin_ss, fin_rs, out_ss, out_rs, cr_ss, cr_rs,
):
    m = lax.axis_index("member")
    f = lax.axis_index("fsdp")
    chips = n // 2
    core = f % 2
    chip = f // 2
    turn = 1 - 2 * core

    def chip_at(place):
        low = place < chips // 2
        return jnp.where(low, 2 * place, 2 * (chips - 1 - place) + 1)

    position = jnp.where(chip % 2 == 0, chip // 2, chips - 1 - chip // 2)

    def place(offset):
        return (position + turn * offset + 2 * chips) % chips

    neighbours = ((m, 2 * chip_at(place(1)) + core), (m, 2 * chip_at(place(-1)) + core))
    hops = (chips // 2, chips - 1 - chips // 2)
    signs = (1, -1)
    twin = (m, 2 * chip + 1 - core)
    partner = (1 - m, f)
    flat = m * n + f
    total = 2 * n

    def device(index):
        return (index // n, index % n)

    barrier = pltpu.get_barrier_semaphore()

    @pl.loop(1, total)
    def greet(k):
        pl.semaphore_signal(barrier, inc=1, device_id=device((flat + k) % total), device_id_type=MESH)

    line = jnp.broadcast_to(noise[...], (8, noise.shape[1]))
    for at, (base, table) in enumerate(((1.0, cond_gain), (0.0, cond_shift))):
        product = jnp.dot(line, table[...], precision=lax.Precision.HIGHEST, preferred_element_type=jnp.float32)
        gs_in[at] = base + product
    pl.semaphore_wait(barrier, total - 1)

    def remote(src, dst, send, recv, to):
        return pltpu.make_async_remote_copy(
            src_ref=src, dst_ref=dst, send_sem=send, recv_sem=recv, device_id=to, device_id_type=MESH
        )

    half = x_s.shape[1]
    width = x_s.shape[2]
    hidden = win_s.shape[1]
    rin = w_in.shape[0]
    rout = w_out.shape[0]
    mine_from = pl.multiple_of(m * half, half)
    other_from = pl.multiple_of((1 - m) * half, half)

    def slot(which, owner):
        if which == 0:
            return win_s.at[pl.ds(pl.multiple_of(owner * rin, rin), rin)]
        return wout_s.at[pl.ds(pl.multiple_of(owner * rout, rout), rout)]

    def ring_copy(which, way, step, src, owner):
        return remote(
            src, slot(which, owner), g_send.at[which, way, step], g_recv.at[which, way, step], neighbours[way]
        )

    def pair_copy(which, way, step, src, owner):
        return remote(src, slot(which, owner), q_send.at[which, way, step], q_recv.at[which, way, step], twin)

    shards = (w_in, w_out)
    for which in range(2):
        for way in range(2):
            ring_copy(which, way, 0, shards[which], f).start()
    swap = remote(lat.at[pl.ds(other_from, half)], x_s.at[0], l_send.at[0], l_recv.at[0], partner)
    swap.start()
    gs_swap = remote(gs_in, gs_s.at[0], l_send.at[1], l_recv.at[1], partner)
    gs_swap.start()
    for which in range(2):
        pair_copy(which, 0, 0, shards[which], f).start()
    keep = pltpu.make_async_copy(lat.at[pl.ds(mine_from, half)], x_s.at[1], local_sem.at[0])
    keep.start()
    goal = pltpu.make_async_copy(target.at[pl.ds(mine_from, half)], t_s, local_sem.at[1])
    goal.start()
    gs_s[1] = gs_in[...]
    cr_s[...] = jnp.zeros_like(cr_s)
    win_s[pl.ds(pl.multiple_of(f * rin, rin), rin), :] = w_in[...]
    wout_s[pl.ds(pl.multiple_of(f * rout, rout), rout), :] = w_out[...]

    passed = []
    for step in range(1, hops[0] + 1):
        for which in range(2):
            for way in range(2):
                if step > hops[way]:
                    continue
                owner = 2 * chip_at(place(-signs[way] * step)) + core
                here = slot(which, owner)
                ring_copy(which, way, step - 1, here, owner).wait_recv()
                if step < hops[way]:
                    onward = ring_copy(which, way, step, here, owner)
                    onward.start()
                    passed.append(onward)
                share = pair_copy(which, way, step, here, owner)
                share.start()
                passed.append(share)
    for which in range(2):
        pair_copy(which, 0, 0, shards[which], 2 * chip + 1 - core).wait_recv()
        for way in range(2):
            for step in range(1, hops[way] + 1):
                owner = 2 * chip_at(place(signs[way] * step)) + 1 - core
                pair_copy(which, way, step, slot(which, owner), owner).wait_recv()
    for which in range(2):
        for way in range(2):
            passed.append(ring_copy(which, way, 0, shards[which], f))
        passed.append(pair_copy(which, 0, 0, shards[which], f))
    for sent in passed:
        sent.wait_send()
    keep.wait()
    goal.wait()
    gs_swap.wait()
    swap.wait()

    tiles = half // TILE
    scale = (1.0 / (2.0 * n * 2 * half) ** 0.5)

    def home(tile):
        start = pl.multiple_of(tile * TILE, TILE)
        there = pl.multiple_of(m * half + tile * TILE, TILE)
        back = remote(p_s.at[0, pl.ds(start, TILE)], pred.at[pl.ds(there, TILE)], p_send.at[tile], p_recv.at[tile], partner)
        here = pltpu.make_async_copy(p_s.at[1, pl.ds(start, TILE)], pred.at[pl.ds(there, TILE)], o_sem.at[tile])
        return back, here

    def arrival(tile):
        start = pl.multiple_of(tile * TILE, TILE)
        there = pl.multiple_of((1 - m) * half + tile * TILE, TILE)
        return remote(p_s.at[0, pl.ds(start, TILE)], pred.at[pl.ds(there, TILE)], p_send.at[tile], p_recv.at[tile], partner)

    @pl.loop(0, tiles)
    def nodes(tile):
        start = pl.multiple_of(tile * TILE, TILE)
        base = pl.multiple_of(tile * 2 * TILE, 2 * TILE)
        rows = pl.ds(base, 2 * TILE)
        for side in range(2):
            values = x_s[side, pl.ds(start, TILE), :].astype(jnp.float32)
            center = jnp.mean(values, axis=1, keepdims=True)
            moved = values - center
            spread = jnp.mean(moved * moved, axis=1, keepdims=True)
            normed = moved * lax.rsqrt(spread + 0.25) * gs_s[side, 0, 0:1, :] + gs_s[side, 1, 0:1, :]
            normed = normed.astype(jnp.bfloat16)
            norm_s[side * TILE : (side + 1) * TILE, :] = normed
        norm_t[:, rows] = norm_s[...].T
        for j in range(hidden // WIDE):
            cols = slice(j * WIDE, (j + 1) * WIDE)
            v = jnp.dot(norm_s[...], win_s[:, cols], preferred_element_type=jnp.float32) + b_in[:, cols]
            square = v * v
            u = jnp.tanh(COEF * (v + CUBIC * square * v))
            gate = 0.5 * (1.0 + u)
            act_s[rows, cols] = (v * gate).astype(jnp.bfloat16)
            slope_s[:, cols] = gate + (0.5 * COEF) * v * (1.0 - u * u) * (1.0 + 3.0 * CUBIC * square)
        out = jnp.dot(act_s[rows, :], wout_s[...], preferred_element_type=jnp.float32)
        guess = []
        for side in range(2):
            value = x_s[side, pl.ds(start, TILE), :].astype(jnp.float32) + out[side * TILE : (side + 1) * TILE]
            value = value.astype(jnp.bfloat16)
            p_s[side, pl.ds(start, TILE), :] = value
            guess.append(value.astype(jnp.float32))
        goal_tile = t_s[pl.ds(start, TILE), :].astype(jnp.float32)
        slopes = []
        value_sum = None
        for d, weight in ((guess[0] - goal_tile, 0.5), (guess[1] - goal_tile, 0.5), (guess[0] - guess[1], -0.5)):
            q = d * d + 0.0625
            r = lax.rsqrt(q)
            slopes.append(0.5 * d * r)
            term = weight * (q * r)
            value_sum = term if value_sum is None else value_sum + term
        cr_s[...] += jnp.sum(value_sum.reshape(TILE // 8, 8, width), axis=0)
        dp_s[:TILE, :] = ((slopes[0] - slopes[2]) * scale).astype(jnp.bfloat16)
        dp_s[TILE:, :] = ((slopes[1] + slopes[2]) * scale).astype(jnp.bfloat16)
        dp_t[:, rows] = dp_s[...].T
        for j in range(hidden // WIDE):
            cols = slice(j * WIDE, (j + 1) * WIDE)
            dact = lax.dot_general(
                dp_s[...], wout_s[cols, :], (((1,), (1,)), ((), ())), preferred_element_type=jnp.float32
            )
            dpre_s[rows, cols] = (dact * slope_s[:, cols]).astype(jnp.bfloat16)
        back, here = home(tile)
        back.start()
        here.start()

    part = cr_s[:, 0:128]
    for j in range(1, width // 128):
        part = part + cr_s[:, j * 128 : (j + 1) * 128]
    cr_tx[...] = part
    cr_rx[flat] = part

    def cr_copy(to, source):
        return remote(cr_tx, cr_rx.at[source], cr_ss.at[to], cr_rs.at[source], device(to))

    cw = hidden // n

    def columns(owner):
        return pl.ds(pl.multiple_of(owner * cw, cw), cw)

    def fin_copy(to, source):
        target_rows = pl.ds(pl.multiple_of((to % n) * rin, rin), rin)
        return remote(gin_tx.at[target_rows], gin_rx.at[source], fin_ss.at[to], fin_rs.at[source], device(to))

    out_copy = remote(gout_tx, gout_rx, out_ss, out_rs, partner)

    def pair_sum(way, step, which):
        at = (way, step, which)
        return remote(pair_tx.at[at], pair_rx.at[at], pair_ss.at[at], pair_rs.at[at], twin)

    def ring_sum(way, step, which):
        at = (way, step, which)
        return remote(ring_tx.at[at], ring_rx.at[at], ring_ss.at[at], ring_rs.at[at], neighbours[way])

    stages = hops[0]

    def compute(step):
        for way in range(2):
            away = signs[way] * (hops[way] - step)
            own = columns(2 * chip_at(place(away)) + core)
            twins = columns(2 * chip_at(place(-away)) + 1 - core)
            for which, (left, right) in enumerate(((norm_t, dpre_s), (dp_t, act_s))):
                both = jnp.concatenate([right[:, own], right[:, twins]], axis=1)
                product = jnp.dot(left[...], both, preferred_element_type=jnp.float32)
                mine_s[way, step, which] = product[:, :cw]
                pair_tx[way, step, which] = product[:, cw:].astype(jnp.bfloat16)
        for way in range(2):
            for which in range(2):
                pair_sum(way, step, which).start()

    def finish(step, first=False, last=False):
        for way in range(2):
            for which in range(2):
                pair_sum(way, step, which).wait_recv()
                value = mine_s[way, step, which] + pair_rx[way, step, which].astype(jnp.float32)
                if not first:
                    ring_sum(way, step - 1, which).wait_recv()
                    value = value + ring_rx[way, step - 1, which].astype(jnp.float32)
                if last and way == 1:
                    ring_sum(0, step, which).wait_recv()
                    value = value + ring_rx[0, step, which].astype(jnp.float32)
                value = value.astype(jnp.bfloat16)
                if not last or way == 0:
                    ring_tx[way, step, which] = value
                    ring_sum(way, step, which).start()
                elif which == 0:
                    gin_tx[...] = value

                    @pl.loop(1, total)
                    def scatter(k):
                        fin_copy((flat + k) % total, flat).start()

                else:
                    gout_tx[...] = value
                    out_copy.start()

    compute(0)
    compute(1)
    finish(0, first=True)

    @pl.loop(1, stages - 1)
    def steps(step):
        compute(step + 1)
        finish(step)

    @pl.loop(1, total)
    def tell(k):
        cr_copy((flat + k) % total, flat).start()

    finish(stages - 1, last=True)

    gin_rx[flat] = gin_tx[pl.ds(pl.multiple_of(f * rin, rin), rin), :]

    @pl.loop(1, total)
    def heard(k):
        cr_copy(flat, (flat + k) % total).wait_recv()

    crps[0, 0] = jnp.sum(jnp.sum(cr_rx[...], axis=0)) / jnp.float32(4 * n * half * width)

    out_copy.wait_recv()
    gout[...] = (gout_tx[...].astype(jnp.float32) + gout_rx[...].astype(jnp.float32)).T

    @pl.loop(1, total)
    def collect(k):
        fin_copy(flat, (flat + k) % total).wait_recv()

    for owner in range(n):
        gin[:, owner * cw : (owner + 1) * cw] = gin_rx[owner].astype(jnp.float32) + gin_rx[n + owner].astype(jnp.float32)

    @pl.loop(0, tiles)
    def settle(tile):
        back, here = home(tile)
        back.wait_send()
        here.wait()
        arrival(tile).wait_recv()

    @pl.loop(0, stages)
    def settle_pair(step):
        for way in range(2):
            for which in range(2):
                pair_sum(way, step, which).wait_send()

    for way in range(2):

        @pl.loop(0, hops[way])
        def settle_ring(step):
            for which in range(2):
                ring_sum(way, step, which).wait_send()

    out_copy.wait_send()

    @pl.loop(1, total)
    def settle_rest(k):
        to = (flat + k) % total
        cr_copy(to, flat).wait_send()
        fin_copy(to, flat).wait_send()


def fits(rows, width, hidden, n):
    return (
        n >= 4
        and n % 4 == 0
        and hidden % n == 0
        and (hidden // n) % 128 == 0
        and width % n == 0
        and (width // n) % 16 == 0
        and width % 128 == 0
        and hidden % WIDE == 0
        and rows % (2 * TILE) == 0
        and rows * hidden <= 2048 * 2048
        and width * hidden <= 512 * 2048
    )


def fused(latents, noise, cond_gain, cond_shift, w_in, b_in, w_out, target):
    block = latents[0]
    rows, width = block.shape
    n = lax.axis_size("fsdp")
    hidden = w_in.shape[1]
    half = rows // 2
    chips = n // 2
    tiles = half // TILE
    cw = hidden // n
    stages = chips // 2
    rin, rout = w_in.shape[0], w_out.shape[0]
    bf, f32 = jnp.bfloat16, jnp.float32
    vmem = pl.BlockSpec(memory_space=pltpu.VMEM)
    anywhere = pl.BlockSpec(memory_space=pl.ANY)
    dma = pltpu.SemaphoreType.DMA
    prediction, grad_in, grad_out, parts = pl.pallas_call(
        functools.partial(fused_kernel, n),
        out_shape=(
            jax.ShapeDtypeStruct((rows, width), bf),
            jax.ShapeDtypeStruct((rin, hidden), f32),
            jax.ShapeDtypeStruct((rout, width), f32),
            jax.ShapeDtypeStruct((1, 1), f32),
        ),
        in_specs=[vmem, vmem, vmem, anywhere, vmem, vmem, vmem, anywhere],
        out_specs=(anywhere, vmem, vmem, pl.BlockSpec(memory_space=pltpu.SMEM)),
        scratch_shapes=[
            pltpu.VMEM((width, hidden), bf),
            pltpu.VMEM((hidden, width), bf),
            pltpu.VMEM((2, half, width), bf),
            pltpu.VMEM((half, width), bf),
            pltpu.VMEM((2, 8, width), f32),
            pltpu.VMEM((2, 2, 8, width), f32),
            pltpu.VMEM((2, half, width), bf),
            pltpu.VMEM((width, rows), bf),
            pltpu.VMEM((2 * TILE, width), bf),
            pltpu.VMEM((rows, hidden), bf),
            pltpu.VMEM((2 * TILE, hidden), f32),
            pltpu.VMEM((2 * TILE, width), bf),
            pltpu.VMEM((width, rows), bf),
            pltpu.VMEM((rows, hidden), bf),
            pltpu.VMEM((8, width), f32),
            pltpu.VMEM((2, stages, 2, width, cw), bf),
            pltpu.VMEM((2, stages, 2, width, cw), bf),
            pltpu.VMEM((2, stages, 2, width, cw), bf),
            pltpu.VMEM((2, stages, 2, width, cw), bf),
            pltpu.VMEM((2, stages, 2, width, cw), f32),
            pltpu.VMEM((width, cw), bf),
            pltpu.VMEM((width, cw), bf),
            pltpu.VMEM((2 * n, rin, cw), bf),
            pltpu.VMEM((width, cw), bf),
            pltpu.VMEM((8, 128), f32),
            pltpu.VMEM((2 * n, 8, 128), f32),
            dma((2, 2, stages + 1)),
            dma((2, 2, stages + 1)),
            dma((2, 2, stages + 1)),
            dma((2, 2, stages + 1)),
            dma((2,)),
            dma((2,)),
            dma((2,)),
            dma((tiles,)),
            dma((tiles,)),
            dma((tiles,)),
            dma((2, stages, 2)),
            dma((2, stages, 2)),
            dma((2, stages, 2)),
            dma((2, stages, 2)),
            dma((2 * n,)),
            dma((2 * n,)),
            dma,
            dma,
            dma((2 * n,)),
            dma((2 * n,)),
        ],
        compiler_params=pltpu.CompilerParams(
            collective_id=0, has_side_effects=True, vmem_limit_bytes=60 * 1024 * 1024
        ),
    )(noise, cond_gain, cond_shift, block, b_in[None, :], w_in, w_out, target)
    crps_mean = parts.reshape(())
    return (prediction[None], grad_in, grad_out, crps_mean)


def on_device(latents, noise, cond_gain, cond_shift, w_in, b_in, w_out, target):
    n = lax.axis_size("fsdp")
    form = fused if fits(latents.shape[1], latents.shape[2], w_in.shape[1], n) else general
    return form(latents, noise, cond_gain, cond_shift, w_in, b_in, w_out, target)


def solution(mesh):
    placed = (
        P("member", "fsdp", None),
        P("member", None),
        P(),
        P(),
        P("fsdp", None),
        P(),
        P("fsdp", None),
        P("fsdp", None),
    )
    return jax.shard_map(
        on_device,
        mesh=mesh,
        in_specs=placed,
        out_specs=(P("member", "fsdp", None), P("fsdp", None), P("fsdp", None), P()),
        check_vma=False,
    )
```
